32 devices in a mesh: row: 4 (over z), col: 4 (over y, x), layer: 2 (over core).
Axes of the slice: x: 2, y: 2, z: 4, core: 2. Of those that a mesh axis runs over, the one named last changes fastest.
Arguments:
- basis: float32 [4096, 4096], P('row', 'col'), may hold values from -1 to 1, as said below
- basis_grad: float32 [4096, 4096], P('row', 'col'), may hold values from -768 to 768
- value_grad: float32 [4096], replicated, may hold values from -384 to 384
- ranks: int32 [4096], replicated, may hold values from 0 to 4095, each once
- offsets: int32 [4096], replicated, may hold values from 0 to 3
Outputs:
- grad_matrix: float32 [4096, 4096], P(('row', 'layer'), 'col')
The draws below stay inside these ranges and needn't reach their ends.
Inputs may be any that keep to these rules, and one draw needn't show every extreme that they name: The columns of basis are orthonormal. ranks holds every number of 0 to 4095 once, so eigenvalues of different indices differ by 1 or more.
All inputs are finite; a program needn't handle non-finite values.
Results may differ from the reference program's by a relative error of at most 0.000098.
Values sent between devices are 32-bit elements; how exact they have to be, the bound alone decides.
A program may use at most 128 MiB of HBM per device.

```python
import jax
import jax.numpy as jnp
from jax import lax

N = 4096


def draw_basis(key, part):
    source = jax.random.normal(key, (N, N), jnp.float32)
    factor, upper = jnp.linalg.qr(source)
    signs = jnp.where(jnp.diagonal(upper) < 0, -1.0, 1.0)
    return (factor * signs[None, :]).astype(jnp.float32)


def with_ends(values, key, low, largest):
    longest = values.shape.index(max(values.shape))
    spots = []
    for shift in (0, 1):
        where = [jax.random.randint(jax.random.fold_in(key, axis), (), 0, length) for axis, length in enumerate(values.shape)]
        where[longest] = (where[longest] + shift) % values.shape[longest]
        spots.append(tuple(where))
    return values.at[spots[0]].set(low).at[spots[1]].set(largest)


def level_of(key, shape, shards, smallest, high):
    gain = 1.0
    for axis_at, blocks in shards:
        draws = jax.random.uniform(jax.random.fold_in(jax.random.fold_in(key, 6), axis_at), (blocks,), jnp.float32, smallest / len(shards), high / len(shards))
        gain = gain * jnp.repeat(jnp.exp(draws), shape[axis_at] // blocks).reshape((-1,) + (1,) * (len(shape) - 1 - axis_at))
    return gain


def noise(key, extent, width, most, shards=(), kind=jnp.bfloat16):
    drawn = jax.random.normal(key, extent, jnp.float32) * width
    if len(shards) > 0:
        drawn = level_of(key, extent, shards, -0.22, 0.18) * drawn
    return jnp.clip(drawn, min=-most, max=most).astype(kind)


def setup_inputs(seed: int = 0) -> dict:
    key_of = jax.random.split(jax.random.key(seed), 6)
    basis = draw_basis(jax.random.fold_in(key_of[5], 71), 0)
    basis_grad = noise(key_of[1], (N, N), (2 * N ** 0.5), 768.0, ((0, 4), (1, 4)), jnp.float32)
    value_grad = noise(key_of[2], (N,), (N ** 0.5), 384.0, (), jnp.float32)
    ranks = jax.random.permutation(key_of[3], N).astype(jnp.int32)
    offsets = with_ends(jax.random.randint(key_of[4], (N,), 0, 4), jax.random.fold_in(key_of[4], 1), 0, 3).astype(jnp.int32)
    return dict(basis=basis, basis_grad=basis_grad, value_grad=value_grad, ranks=ranks, offsets=offsets)


def reference(basis, basis_grad, value_grad, ranks, offsets):
    highest = lax.Precision.HIGHEST
    eigen = 4.0 * ranks.astype(jnp.float32) + offsets.astype(jnp.float32)
    inner = jnp.dot(basis.T.astype(jnp.float32), basis_grad.astype(jnp.float32), precision=highest, preferred_element_type=jnp.float32)
    index = jnp.arange(N, dtype=jnp.int32)
    on_diagonal = index[:, None] == index[None, :]
    spacing = eigen[None, :] - eigen[:, None]
    scaled = jnp.where(on_diagonal, value_grad[None, :], inner / jnp.where(on_diagonal, jnp.float32(1.0), spacing))
    left_prod = jnp.dot(basis.astype(jnp.float32), scaled.astype(jnp.float32), precision=highest, preferred_element_type=jnp.float32)
    return jnp.dot(left_prod.astype(jnp.float32), basis.T.astype(jnp.float32), precision=highest, preferred_element_type=jnp.float32)
```

```python
import functools

import jax
import jax.numpy as jnp
from jax import lax
from jax.experimental import pallas as pl
from jax.experimental.pallas import tpu as pltpu
from jax.sharding import PartitionSpec as P


MESH = pl.DeviceIdType.MESH
CHUNKS = 4
ROUNDS = 4
VMEM_BYTES = 63 * 1024 * 1024


def send(src, dst, send_sem, recv_sem, where):
    return pltpu.make_async_remote_copy(
        src_ref=src, dst_ref=dst, send_sem=send_sem, recv_sem=recv_sem, device_id=where, device_id_type=MESH
    )


def greet(places):
    barrier = pltpu.get_barrier_semaphore()
    for where in places:
        pl.semaphore_signal(barrier, inc=1, device_id=where, device_id_type=MESH)
    pl.semaphore_wait(barrier, len(places))


def split(v):
    high = v.astype(jnp.bfloat16)
    return high, (v - high.astype(jnp.float32)).astype(jnp.bfloat16)


def mm(a, b, dims):
    return lax.dot_general(a, b, (dims, ((), ())), preferred_element_type=jnp.float32)


def mm3(a_hi, a_lo, b_hi, b_lo, dims):
    return mm(a_hi, b_hi, dims) + (mm(a_hi, b_lo, dims) + mm(a_lo, b_hi, dims))


NN = ((1,), (0,))
NT = ((1,), (1,))


def place(nr):
    z, c, l = lax.axis_index("row"), lax.axis_index("col"), lax.axis_index("layer")
    return z, c // 2, c % 2, l


def at(z, y, x, l):
    return {"row": z, "col": 2 * y + x, "layer": l}


def first_kernel(nr, q_ref, g_ref, e_ref, v_ref, qh_out, ql_out, sh_out, sl_out,
                 qbuf, gbuf, qh, ql, acc, q_in, up_out, down_out, x_out, h_sem, l_sem,
                 gz_out, gz_in, gy_out, gy_in, gl_out, gl_in):
    z, y, x, l = place(nr)
    lead = l == x
    block, cols = q_ref.shape
    rows = block // CHUNKS
    width = cols // nr
    same = [at(lax.rem(z + d, nr), y, x, l) for d in range(1, nr)]
    across, beside, mate = at(z, y, 1 - x, l), at(z, 1 - y, x, l), at(z, y, x, 1 - l)
    greet(same + [across, beside, mate])

    def local_q(ch):
        part = pl.ds(ch * rows, rows)
        return pltpu.make_async_copy(q_ref.at[part], qbuf.at[z, part], q_in.at[z, ch])

    def pass_q(s, b, ch, out, where, own):
        part = pl.ds(pl.multiple_of(ch * rows, rows), rows)
        src = q_ref.at[part] if own else qbuf.at[b, part]
        return send(src, qbuf.at[b, part], out.at[s, ch], q_in.at[b, ch], where)

    def up(s, b, ch, own=False):
        return pass_q(s, b, ch, up_out, at(z + 1, y, x, l), own)

    def down(s, b, ch, own=False):
        return pass_q(s, b, ch, down_out, at(z - 1, y, x, l), own)

    def side(b, ch, own=False):
        return pass_q(b, b, ch, x_out, across, own)

    def await_q(b, ch):
        part = pl.ds(pl.multiple_of(ch * rows, rows), rows)
        pltpu.make_async_copy(q_ref.at[part], qbuf.at[b, part], q_in.at[b, ch]).wait()

    def own_g(k):
        return g_ref.at[:, pl.ds(pl.multiple_of(k * width, width), width)]

    def z_g(k):
        return send(own_g(k), gbuf.at[z, y], gz_out.at[k], gz_in.at[z], at(k, y, x, l))

    def y_g(b, src):
        return send(src, gbuf.at[b, y], gy_out.at[b], gy_in.at[b], beside)

    def mate_g(b, h, src):
        return send(src, gbuf.at[b, h], gl_out.at[b, h], gl_in.at[b, h], mate)

    def own_g_copy():
        return pltpu.make_async_copy(own_g(z), gbuf.at[z, y], gz_in.at[z])

    def await_z_g(b):
        pltpu.make_async_copy(own_g(0), gbuf.at[b, y], gz_in.at[b]).wait()

    def await_y_g(b):
        pltpu.make_async_copy(own_g(0), gbuf.at[b, 1 - y], gy_in.at[b]).wait()

    @pl.when(lead)
    def _():
        for ch in range(CHUNKS):
            pl.when(z < nr - 1)(lambda ch=ch: up(0, z, ch, True).start())
            pl.when(z > 0)(lambda ch=ch: down(0, z, ch, True).start())
            side(z, ch, True).start()
            local_q(ch).start()

    @pl.when(jnp.logical_not(lead))
    def _():
        y_g(z, own_g(z)).start()
        mate_g(z, y, own_g(z)).start()
        own_g_copy().start()
        for d in range(1, nr):
            pl.when(z + d < nr)(lambda d=d: z_g(z + d).start())
            pl.when(z - d >= 0)(lambda d=d: z_g(z - d).start())
        await_y_g(z)
        mate_g(z, 1 - y, gbuf.at[z, 1 - y]).start()
        for d in range(1, nr):
            for step in (-d, d):
                b = z + step

                @pl.when(jnp.logical_and(b >= 0, b < nr))
                def _(b=b):
                    await_z_g(b)
                    y_g(b, gbuf.at[b, y]).start()
                    mate_g(b, y, gbuf.at[b, y]).start()
            for step in (-d, d):
                b = z + step

                @pl.when(jnp.logical_and(b >= 0, b < nr))
                def _(b=b):
                    await_y_g(b)
                    mate_g(b, 1 - y, gbuf.at[b, 1 - y]).start()
        await_z_g(z)

    acc[...] = jnp.zeros_like(acc)

    def absorb(s, b, ch):
        part = pl.ds(pl.multiple_of(ch * rows, rows), rows)

        @pl.when(jnp.logical_or(jnp.logical_not(lead), s == 0))
        def _():
            await_q(b, ch)

        @pl.when(jnp.logical_and(lead, ch == 0))
        def _():
            for h in range(2):
                pltpu.make_async_copy(own_g(0), gbuf.at[b, h], gl_in.at[b, h]).wait()

        high, low = split(qbuf[b, part, :])
        qh[b, part, :] = high
        ql[b, part, :] = low
        pltpu.make_async_copy(qh.at[b, part], qh_out.at[b, part], h_sem.at[b, ch]).start()
        pltpu.make_async_copy(ql.at[b, part], ql_out.at[b, part], l_sem.at[b, ch]).start()
        for h in range(2):
            g_hi, g_lo = split(gbuf[b, h, part, :].T)
            acc[h] += mm3(g_hi, g_lo, high, low, NN)

    def forward(s, ch):
        @pl.when(jnp.logical_and(lead, z >= s))
        def _():
            await_q(z - s, ch)
            pl.when(z < nr - 1)(lambda: up(s, z - s, ch).start())
            side(z - s, ch).start()

        @pl.when(jnp.logical_and(lead, z + s < nr))
        def _():
            await_q(z + s, ch)
            pl.when(z > 0)(lambda: down(s, z + s, ch).start())
            side(z + s, ch).start()

    def absorb_at(s, ch):
        pl.when(z >= s)(lambda: absorb(s, z - s, ch))
        if s > 0:
            pl.when(z + s < nr)(lambda: absorb(s, z + s, ch))

    for s in range(1, nr):
        def step(ch, carry, s=s):
            forward(s, ch)
            absorb_at(s - 1, ch)
            if s == nr - 1:
                absorb_at(s, ch)
            return carry

        lax.fori_loop(0, CHUNKS, step, 0)

    vec_i = e_ref[2 * y + l]
    i_at = (2 * y + l) * cols + lax.broadcasted_iota(jnp.int32, (width, cols), 1)
    for h in range(2):
        j_cols = pl.ds(pl.multiple_of(z * width, width), width)
        upright = lambda v: jnp.broadcast_to(v, (128, width)).T[:, :1]
        e_j, v_j = upright(e_ref[2 * h + x, :, j_cols]), upright(v_ref[2 * h + x, :, j_cols])
        j_at = (2 * h + x) * cols + z * width + lax.broadcasted_iota(jnp.int32, (width, cols), 0)
        on = i_at == j_at
        spacing = jnp.where(on, jnp.float32(1.0), e_j - vec_i)
        scaled = jnp.where(on, v_j, acc[h] / spacing)
        high, low = split(scaled)
        sh_out[h] = high
        sl_out[h] = low

    @pl.when(lead)
    def _():
        def drain(t, carry):
            ch = t
            for s in range(nr):
                @pl.when(jnp.logical_and(z >= s, z < nr - 1))
                def _(s=s):
                    up(s, z - s, ch).wait_send()

                @pl.when(jnp.logical_and(z + s < nr, z > 0))
                def _(s=s):
                    down(s, z + s, ch).wait_send()
                side(s, ch).wait_send()
            return carry

        lax.fori_loop(0, CHUNKS, drain, 0)

    @pl.when(jnp.logical_not(lead))
    def _():
        for b in range(nr):
            y_g(b, gbuf.at[b, y]).wait_send()
            for h in range(2):
                mate_g(b, h, gbuf.at[b, h]).wait_send()
            pl.when(z != b)(lambda b=b: z_g(b).wait_send())

    def settle(t, carry):
        for b in range(nr):
            part = pl.ds(pl.multiple_of(t * rows, rows), rows)
            pltpu.make_async_copy(qh.at[b, part], qh_out.at[b, part], h_sem.at[b, t]).wait()
            pltpu.make_async_copy(ql.at[b, part], ql_out.at[b, part], l_sem.at[b, t]).wait()
        return carry

    lax.fori_loop(0, CHUNKS, settle, 0)


def second_kernel(nr, qh_ref, ql_ref, sh_ref, sl_ref, out_ref,
                  qh, ql, part, mate_in, beside_in, left_in, total, total_in, total_y,
                  qh_sem, ql_sem, lm_out, lm_in, ly_out, ly_in, lz_out, lz_in,
                  om_out, om_in, oy_out, oy_in, end_out, end_in):
    z, y, x, l = place(nr)
    lead = l == x
    cols = qh.shape[-1]
    rows = qh.shape[3]
    width = cols // nr
    beside, mate = at(z, 1 - y, x, l), at(z, y, x, 1 - l)
    goal = lambda k: at(k, y, l, x)

    def load(r):
        return [
            pltpu.make_async_copy(qh_ref.at[:, :, r], qh.at[r], qh_sem.at[r]),
            pltpu.make_async_copy(ql_ref.at[:, :, r], ql.at[r], ql_sem.at[r]),
        ]

    for r in range(ROUNDS):
        for copy in load(r):
            copy.start()

    @pl.when(lead)
    def _():
        greet([goal(lax.rem(z + d, nr)) for d in range(1, nr)] + [beside, mate])

    @pl.when(jnp.logical_not(lead))
    def _():
        greet([goal(lax.rem(z + d, nr)) for d in range(nr)] + [beside, mate])

    def left_mate(r):
        return send(part.at[r, 1 - l], mate_in.at[r], lm_out.at[r], lm_in.at[r], mate)

    def left_beside(r):
        return send(part.at[r, l, 1 - y], beside_in.at[r], ly_out.at[r], ly_in.at[r], beside)

    def left_goal(r, k):
        return send(beside_in.at[r, k], left_in.at[r, z], lz_out.at[r, k], lz_in.at[r, z], goal(k))

    def left_here(r):
        return pltpu.make_async_copy(beside_in.at[r, z], left_in.at[r, z], lz_in.at[r, z])

    def total_mate(r):
        return send(total.at[r, 1 - l], total_in.at[r], om_out.at[r], om_in.at[r], mate)

    def total_beside(r):
        return send(total.at[r, l, 1 - y], total_y.at[r], oy_out.at[r], oy_in.at[r], beside)

    def end_there(r):
        spot = out_ref.at[pl.ds(pl.multiple_of(r * rows, rows), rows)]
        return send(total_y.at[r], spot, end_out.at[r], end_in.at[r], at(z, y, l, x))

    def end_here(r):
        spot = out_ref.at[pl.ds(pl.multiple_of(r * rows, rows), rows)]
        return pltpu.make_async_copy(total_y.at[r], spot, end_in.at[r])

    def left(r):
        for copy in load(r):
            copy.wait()

        def half(lr):
            a_hi = qh[r, :, lr].reshape(nr * rows, cols)
            a_lo = ql[r, :, lr].reshape(nr * rows, cols)
            for h in range(2):
                part[r, lr, h] = mm3(a_hi, a_lo, sh_ref[h], sl_ref[h], NT).reshape(nr, rows, width)

        half(1 - l)
        left_mate(r).start()
        half(l)

    def left_sum(r):
        left_mate(r).wait_recv()
        part[r, l, 1 - y] += mate_in[r, 1 - y]
        left_beside(r).start()

    def left_end(r):
        left_beside(r).wait_recv()
        beside_in[r] += part[r, l, y] + mate_in[r, y]
        for k in range(nr):
            away = jnp.logical_or(jnp.logical_not(lead), z != k)
            pl.when(away)(lambda k=k: left_goal(r, k).start())
        pl.when(lead)(lambda: left_here(r).start())

    def grad(r):
        for k in range(nr):
            pltpu.make_async_copy(beside_in.at[r, k], left_in.at[r, k], lz_in.at[r, k]).wait()
        a_hi, a_lo = split(jnp.concatenate([left_in[r, k] for k in range(nr)], axis=1))
        size = ROUNDS * rows

        def half(xx):
            for h in range(2):
                for lr in range(2):
                    b_hi = qh[:, 2 * h + xx, lr].reshape(size, cols)
                    b_lo = ql[:, 2 * h + xx, lr].reshape(size, cols)
                    total[r, xx, h, :, lr * size:(lr + 1) * size] = mm3(a_hi, a_lo, b_hi, b_lo, NT)

        half(1 - l)
        total_mate(r).start()
        half(l)

    def grad_sum(r):
        total_mate(r).wait_recv()
        total[r, l, 1 - y] += total_in[r, 1 - y]
        total_beside(r).start()

    def grad_end(r):
        total_beside(r).wait_recv()
        total_y[r] += total[r, l, y] + total_in[r, y]
        pl.when(lead)(lambda: end_here(r).start())
        pl.when(jnp.logical_not(lead))(lambda: end_there(r).start())

    def one(r, carry):
        pl.when(r < ROUNDS)(lambda: left(r))
        pl.when(r >= 1)(lambda: left_sum(r - 1))
        return carry

    def two(r, carry):
        pl.when(r < ROUNDS)(lambda: left_end(r))
        pl.when(jnp.logical_and(r >= 1, r <= ROUNDS))(lambda: grad(r - 1))
        pl.when(r >= 2)(lambda: grad_sum(r - 2))
        return carry

    def three(r, carry):
        grad_end(r)
        return carry

    def drain(r, carry):
        left_mate(r).wait_send()
        left_beside(r).wait_send()
        for k in range(nr):
            away = jnp.logical_or(jnp.logical_not(lead), z != k)
            pl.when(away)(lambda k=k: left_goal(r, k).wait_send())
        total_mate(r).wait_send()
        total_beside(r).wait_send()
        pl.when(jnp.logical_not(lead))(lambda: end_there(r).wait_send())
        end_here(r).wait()
        return carry

    lax.fori_loop(0, ROUNDS + 1, one, 0)
    lax.fori_loop(0, ROUNDS + 2, two, 0)
    lax.fori_loop(0, ROUNDS, three, 0)
    lax.fori_loop(0, ROUNDS, drain, 0)


def chip_pairs(basis, basis_grad, value_grad, ranks, offsets):
    nr, nc = lax.axis_size("row"), lax.axis_size("col")
    block, cols = basis.shape
    width = cols // nr
    rows = block // 2 // ROUNDS
    eigen = (4.0 * ranks.astype(jnp.float32) + offsets.astype(jnp.float32)).reshape(nc, 1, cols)
    f32, bf16, dma = jnp.float32, jnp.bfloat16, pltpu.SemaphoreType.DMA
    anywhere, vmem = pl.BlockSpec(memory_space=pl.ANY), pl.BlockSpec(memory_space=pltpu.VMEM)
    shape = jax.ShapeDtypeStruct
    whole = (nr, block, cols)
    qh, ql, sh, sl = pl.pallas_call(
        functools.partial(first_kernel, nr),
        out_shape=[shape(whole, bf16)] * 2 + [shape((2, width, cols), bf16)] * 2,
        in_specs=[anywhere, anywhere, vmem, vmem],
        out_specs=[anywhere, anywhere, vmem, vmem],
        scratch_shapes=[
            pltpu.VMEM(whole, f32), pltpu.VMEM((nr, 2, block, width), f32),
            pltpu.VMEM(whole, bf16), pltpu.VMEM(whole, bf16), pltpu.VMEM((2, width, cols), f32),
            dma((nr, CHUNKS)), dma((nr, CHUNKS)), dma((nr, CHUNKS)), dma((nr, CHUNKS)),
            dma((nr, CHUNKS)), dma((nr, CHUNKS)),
            dma((nr,)), dma((nr,)), dma((nr,)), dma((nr,)), dma((nr, 2)), dma((nr, 2)),
        ],
        compiler_params=pltpu.CompilerParams(
            collective_id=0, has_side_effects=True, vmem_limit_bytes=VMEM_BYTES
        ),
        name="first",
    )(basis, basis_grad, eigen, value_grad.reshape(nc, 1, cols))
    order = (nr, 2, ROUNDS, rows, cols)
    kept = (ROUNDS, nr, 2, rows, cols)
    piece = (ROUNDS, nr, rows, width)
    return pl.pallas_call(
        functools.partial(second_kernel, nr),
        out_shape=shape((block // 2, cols), f32),
        in_specs=[anywhere, anywhere, vmem, vmem],
        out_specs=anywhere,
        scratch_shapes=[
            pltpu.VMEM(kept, bf16), pltpu.VMEM(kept, bf16),
            pltpu.VMEM((ROUNDS, 2, 2, nr, rows, width), f32), pltpu.VMEM((ROUNDS, 2, nr, rows, width), f32),
            pltpu.VMEM(piece, f32), pltpu.VMEM(piece, f32),
            pltpu.VMEM((ROUNDS, 2, 2, rows, cols), f32), pltpu.VMEM((ROUNDS, 2, rows, cols), f32),
            pltpu.VMEM((ROUNDS, rows, cols), f32),
            dma((ROUNDS,)), dma((ROUNDS,)), dma((ROUNDS,)), dma((ROUNDS,)), dma((ROUNDS,)), dma((ROUNDS,)),
            dma((ROUNDS, nr)), dma((ROUNDS, nr)),
            dma((ROUNDS,)), dma((ROUNDS,)), dma((ROUNDS,)), dma((ROUNDS,)), dma((ROUNDS,)), dma((ROUNDS,)),
        ],
        compiler_params=pltpu.CompilerParams(
            collective_id=1, has_side_effects=True, vmem_limit_bytes=VMEM_BYTES
        ),
        name="second",
    )(qh.reshape(order), ql.reshape(order), sh, sl)


def dot(a, b, dims):
    return lax.dot_general(
        a, b, (dims, ((), ())), precision=lax.Precision.HIGH, preferred_element_type=jnp.float32
    )


def flip(v, axis, q):
    n = lax.axis_size(axis)
    return lax.ppermute(v, axis, [(i, i ^ q) for i in range(n)])


def shift(v, axis, d):
    if d == 0:
        return v
    n = lax.axis_size(axis)
    return lax.ppermute(v, axis, [(i, (i + d) % n) for i in range(n)])


def gather_begin(v):
    n = lax.axis_size("col")
    if n != 4:
        return [flip(v, "col", q) for q in range(1, n)]
    half = v.shape[0] // 2
    a, b = v[:half], v[half:]
    return [flip(a, "col", 1), flip(b, "col", 2), flip(a, "col", 2), flip(b, "col", 1)]


def gather_end(v, first):
    if lax.axis_size("col") != 4:
        return [v] + first
    a1, b2, a2, b1 = first
    a3, b3 = flip(a1, "col", 2), flip(b2, "col", 1)
    return [v] + [jnp.concatenate(pair) for pair in ((a1, b1), (a2, b2), (a3, b3))]


def scatter_cols(part, rows):
    n = lax.axis_size("col")
    order = (3, 1, 2, 0) if n == 4 else tuple(range(1, n)) + (0,)
    term = {q: lax.optimization_barrier(part(q)) for q in order}
    if n != 4:
        moved = [flip(term[q], "col", q) for q in range(1, n)]
        total = term[0]
        for v in moved:
            total = total + v
        return total, moved[0]
    half = rows // 2
    pa = {q: v[:half] for q, v in term.items()}
    pb = {q: v[half:] for q, v in term.items()}
    moved = flip(pa[3], "col", 1)
    a2 = pa[2] + moved
    b1 = pb[1] + flip(pb[3], "col", 2)
    a0 = pa[0] + flip(pa[1], "col", 1)
    b0 = pb[0] + flip(pb[2], "col", 2)
    return jnp.concatenate([a0 + flip(a2, "col", 2), b0 + flip(b1, "col", 1)]), moved


def swap_layers(mine, axis):
    if lax.axis_size("layer") != 2:
        return lax.all_gather(mine, "layer", axis=axis, tiled=True)
    other = flip(mine, "layer", 1)
    first = lax.axis_index("layer") == 0
    return jnp.concatenate([jnp.where(first, mine, other), jnp.where(first, other, mine)], axis=axis)


def on_device(basis, basis_grad, value_grad, ranks, offsets):
    rows_blk, cols_blk = basis.shape
    nr, nc, nl = (lax.axis_size(a) for a in ("row", "col", "layer"))
    row_id, col_id, layer_id = (lax.axis_index(a) for a in ("row", "col", "layer"))
    width = cols_blk // (nr * nl)
    half = rows_blk // nl

    pieces = [None] * nr
    for d in range(nr):
        begin = (lax.rem(row_id + d, nr) * nl + layer_id) * width
        piece = lax.dynamic_slice_in_dim(basis_grad, begin, width, 1)
        pieces[(nr - d) % nr] = shift(piece, "row", d)

    mine = lax.dynamic_slice_in_dim(basis, layer_id * half, half, 0)
    up, down = [mine], [mine]
    for s in range(1, nr):
        up.append(lax.ppermute(up[-1], "row", [(i, i + 1) for i in range(s - 1, nr - 1)]))
        down.append(lax.ppermute(down[-1], "row", [(i, i - 1) for i in range(1, nr - s + 1)]))
        if s == 1:
            up[1], down[1], pieces = lax.optimization_barrier((up[1], down[1], pieces))
            pieces = jnp.concatenate(pieces)
            begun = gather_begin(pieces)
        if s == 2:
            up[2], down[2], begun = lax.optimization_barrier((up[2], down[2], begun))
    cotangent = jnp.concatenate(gather_end(pieces, begun), axis=1).reshape(nr, rows_blk, nc * width)
    vectors = [basis]
    for e in range(1, nr):
        block = jnp.where(row_id + e < nr, down[e], up[nr - e])
        vectors.append(swap_layers(block, 0))

    inner = dot(vectors[0], cotangent[0], ((0,), (0,)))
    for e in sorted(range(1, nr), key=lambda e: min(e, nr - e)):
        inner = inner + dot(vectors[e], cotangent[e], ((0,), (0,)))

    eigen = 4.0 * ranks.astype(jnp.float32) + offsets.astype(jnp.float32)
    place = row_id * nl + layer_id

    def columns(v):
        mine = lax.dynamic_index_in_dim(v.reshape(nc, nr * nl, width), place, 1, keepdims=False)
        return jnp.concatenate([lax.dynamic_index_in_dim(mine, col_id ^ q, 0, keepdims=False) for q in range(nc)])

    row_index = col_id * cols_blk + jnp.arange(cols_blk, dtype=jnp.int32)
    col_index = columns(jnp.arange(nc * cols_blk, dtype=jnp.int32))
    eigen_rows = lax.dynamic_slice_in_dim(eigen, col_id * cols_blk, cols_blk, 0)
    on_diagonal = row_index[:, None] == col_index[None, :]
    spacing = columns(eigen)[None, :] - eigen_rows[:, None]
    scaled = jnp.where(
        on_diagonal, columns(value_grad)[None, :], inner / jnp.where(on_diagonal, jnp.float32(1.0), spacing)
    )

    arrived = [None] * nr
    order = sorted(range(nr), key=lambda e: -min(e, nr - e))
    groups = [g for g in (order[:nr // 2 - 1], order[nr // 2 - 1:nr - 1], order[nr - 1:]) if g]
    factor = scaled
    for group in groups:
        product = dot(jnp.concatenate([vectors[e] for e in group]), factor, ((1,), (0,)))
        product = lax.optimization_barrier(product)
        summed, first = scatter_cols(lambda q: product[:, q * width:(q + 1) * width], product.shape[0])
        factor, first = lax.optimization_barrier((factor, first))
        for i, e in enumerate(group):
            arrived[e] = shift(summed[i * rows_blk:(i + 1) * rows_blk], "row", e)
    own = []
    for e in range(nr):
        keep = lax.dynamic_slice_in_dim(arrived[e], layer_id * half, half, 0)
        if nl == 1:
            own.append(keep)
            continue
        give = lax.dynamic_slice_in_dim(arrived[e], (1 - layer_id) * half, half, 0)
        other = flip(give, "layer", 1)
        first = layer_id == 0
        own.append(jnp.concatenate([jnp.where(first, keep, other), jnp.where(first, other, keep)], axis=1))
    own = jnp.stack(own)
    left = jnp.concatenate(
        [lax.dynamic_index_in_dim(own, lax.rem(row_id - r + nr, nr), 0, keepdims=False) for r in range(nr)], axis=1
    )

    stack = jnp.stack(vectors)

    def grad_part(q):
        e = lax.rem((col_id ^ q) - row_id + nr, nr)
        block = lax.dynamic_index_in_dim(stack, e, 0, keepdims=False)
        return dot(left, block, ((1,), (1,)))

    return scatter_cols(grad_part, half)[0]


def solution(mesh):
    placed = (P("row", "col"), P("row", "col"), P(), P(), P())
    pairs = (mesh.shape["row"], mesh.shape["col"], mesh.shape["layer"]) == (4, 4, 2)
    return jax.shard_map(
        chip_pairs if pairs else on_device, mesh=mesh, in_specs=placed, out_specs=P(("row", "layer"), "col"), check_vma=False
    )
```

```python
import functools

import jax
import jax.numpy as jnp
from jax import lax
from jax.experimental import pallas as pl
from jax.experimental.pallas import tpu as pltpu
from jax.sharding import PartitionSpec as P


MESH = pl.DeviceIdType.MESH
CHUNKS = 4
GRAINS = 4
ROUNDS = 4
FOLD = GRAINS // ROUNDS
VMEM_BYTES = 63 * 1024 * 1024


def send(src, dst, send_sem, recv_sem, where):
    return pltpu.make_async_remote_copy(
        src_ref=src, dst_ref=dst, send_sem=send_sem, recv_sem=recv_sem, device_id=where, device_id_type=MESH
    )


def greet(places):
    barrier = pltpu.get_barrier_semaphore()
    for where in places:
        pl.semaphore_signal(barrier, inc=1, device_id=where, device_id_type=MESH)
    pl.semaphore_wait(barrier, len(places))


def split(v):
    high = v.astype(jnp.bfloat16)
    return high, (v - high.astype(jnp.float32)).astype(jnp.bfloat16)


def mm(a, b, dims):
    return lax.dot_general(a, b, (dims, ((), ())), preferred_element_type=jnp.float32)


def mm3(a_hi, a_lo, b_hi, b_lo, dims):
    return mm(a_hi, b_hi, dims) + (mm(a_hi, b_lo, dims) + mm(a_lo, b_hi, dims))


NN = ((1,), (0,))
NT = ((1,), (1,))


def place(nr):
    z, c, l = lax.axis_index("row"), lax.axis_index("col"), lax.axis_index("layer")
    return z, c // 2, c % 2, l


def at(z, y, x, l):
    return {"row": z, "col": 2 * y + x, "layer": l}


def chip_kernel(nr, q_ref, g_ref, ranks_ref, offsets_ref, v_ref, out_ref,
                qbuf, gbuf, qh, ql, acc, sh, sl, mate_in, beside_in, left_in, total_in, total_y,
                q_in, up_out, down_out, x_out, gz_out, gz_in, gy_out, gy_in, gl_out, gl_in,
                lm_out, lm_in, ly_out, ly_in, lz_out, lz_in, om_out, om_in, ox_out, ox_in, oy_out, oy_in, end_out):
    z, y, x, l = place(nr)
    lead = l == x
    other = jnp.logical_not(lead)
    block, cols = q_ref.shape
    rows = block // CHUNKS
    width = cols // nr
    half = block // 2
    thin, wide = half // GRAINS, half // ROUNDS
    across, beside, mate = at(z, y, 1 - x, l), at(z, 1 - y, x, l), at(z, y, x, 1 - l)
    goal = lambda k: at(k, y, l, x)
    line = [at(lax.rem(z + d, nr), y, x, l) for d in range(1, nr)] + [across, beside, mate]
    pl.when(lead)(lambda: greet(line))
    pl.when(other)(lambda: greet(line + [goal(lax.rem(z + d, nr)) for d in range(nr)]))

    def span(start, size):
        return pl.ds(pl.multiple_of(start, size), size)

    def local_q(ch):
        return pltpu.make_async_copy(
            q_ref.at[span(ch * rows, rows)], qbuf.at[span(z * block + ch * rows, rows)], q_in.at[z, ch]
        )

    def pass_q(s, b, ch, out, where, own):
        spot = qbuf.at[span(b * block + ch * rows, rows)]
        src = q_ref.at[span(ch * rows, rows)] if own else spot
        return send(src, spot, out.at[s, ch], q_in.at[b, ch], where)

    def up(s, b, ch, own=False):
        return pass_q(s, b, ch, up_out, at(z + 1, y, x, l), own)

    def down(s, b, ch, own=False):
        return pass_q(s, b, ch, down_out, at(z - 1, y, x, l), own)

    def side(b, ch, own=False):
        return pass_q(b, b, ch, x_out, across, own)

    def await_q(b, ch):
        pltpu.make_async_copy(
            q_ref.at[span(ch * rows, rows)], qbuf.at[span(b * block + ch * rows, rows)], q_in.at[b, ch]
        ).wait()

    def slot(b, h):
        return gbuf.at[span(b * block, block), span(h * width, width)]

    def own_g(k):
        return g_ref.at[:, span(k * width, width)]

    def z_g(k):
        return send(own_g(k), slot(z, y), gz_out.at[k], gz_in.at[z], at(k, y, x, l))

    def y_g(b, src):
        return send(src, slot(b, y), gy_out.at[b], gy_in.at[b], beside)

    def mate_g(b, h, src):
        return send(src, slot(b, h), gl_out.at[b, h], gl_in.at[b, h], mate)

    def own_g_copy():
        return pltpu.make_async_copy(own_g(z), slot(z, y), gz_in.at[z])

    def await_z_g(b):
        pltpu.make_async_copy(own_g(0), slot(b, y), gz_in.at[b]).wait()

    def await_y_g(b):
        pltpu.make_async_copy(own_g(0), slot(b, 1 - y), gy_in.at[b]).wait()

    @pl.when(lead)
    def _():
        for ch in range(CHUNKS):
            side(z, ch, True).start()
            pl.when(z < nr - 1)(lambda ch=ch: up(0, z, ch, True).start())
            pl.when(z > 0)(lambda ch=ch: down(0, z, ch, True).start())
            local_q(ch).start()

    @pl.when(other)
    def _():
        for d in range(1, nr):
            pl.when(z + d < nr)(lambda d=d: z_g(z + d).start())
            pl.when(z - d >= 0)(lambda d=d: z_g(z - d).start())
        y_g(z, own_g(z)).start()
        mate_g(z, y, own_g(z)).start()
        own_g_copy().start()
        await_y_g(z)
        mate_g(z, 1 - y, slot(z, 1 - y)).start()
        for d in range(1, nr):
            for step in (-d, d):
                b = z + step

                @pl.when(jnp.logical_and(b >= 0, b < nr))
                def _(b=b):
                    await_z_g(b)
                    y_g(b, slot(b, y)).start()
                    mate_g(b, y, slot(b, y)).start()
            for step in (-d, d):
                b = z + step

                @pl.when(jnp.logical_and(b >= 0, b < nr))
                def _(b=b):
                    await_y_g(b)
                    mate_g(b, 1 - y, slot(b, 1 - y)).start()
        await_z_g(z)

    acc[...] = jnp.zeros_like(acc)

    def absorb(s, b, ch):
        pl.when(jnp.logical_or(other, s == 0))(lambda: await_q(b, ch))

        @pl.when(jnp.logical_and(lead, ch == 0))
        def _():
            for h in range(2):
                pltpu.make_async_copy(own_g(0), slot(b, h), gl_in.at[b, h]).wait()

        part, taken = span(ch * rows, rows), span(b * block + ch * rows, rows)
        high, low = split(qbuf[taken, :])
        qh[b, part, :] = high
        ql[b, part, :] = low
        for h in range(2):
            g_hi, g_lo = split(gbuf[taken, h * width:(h + 1) * width].T)
            acc[h] += mm3(g_hi, g_lo, high, low, NN)

    def forward(s, ch):
        @pl.when(jnp.logical_and(lead, z >= s))
        def _():
            await_q(z - s, ch)
            pl.when(z < nr - 1)(lambda: up(s, z - s, ch).start())
            side(z - s, ch).start()

        @pl.when(jnp.logical_and(lead, z + s < nr))
        def _():
            await_q(z + s, ch)
            pl.when(z > 0)(lambda: down(s, z + s, ch).start())
            side(z + s, ch).start()

    def absorb_at(s, ch):
        pl.when(z >= s)(lambda: absorb(s, z - s, ch))
        if s > 0:
            pl.when(z + s < nr)(lambda: absorb(s, z + s, ch))

    for s in range(1, nr):
        def step(ch, carry, s=s):
            forward(s, ch)
            absorb_at(s - 1, ch)
            if s == nr - 1:
                absorb_at(s, ch)
            return carry

        lax.fori_loop(0, CHUNKS, step, 0)

    def eigen(k, where):
        return 4.0 * ranks_ref[k, :, where].astype(jnp.float32) + offsets_ref[k, :, where].astype(jnp.float32)

    e_i = eigen(2 * y + l, slice(None))
    i_at = (2 * y + l) * cols + lax.broadcasted_iota(jnp.int32, (width, cols), 1)
    for h in range(2):
        j_cols = span(z * width, width)
        upright = lambda v: jnp.broadcast_to(v, (128, width)).T[:, :1]
        e_j, v_j = upright(eigen(2 * h + x, j_cols)), upright(v_ref[2 * h + x, :, j_cols])
        j_at = (2 * h + x) * cols + z * width + lax.broadcasted_iota(jnp.int32, (width, cols), 0)
        on = i_at == j_at
        spacing = jnp.where(on, jnp.float32(1.0), e_j - e_i)
        sh[h], sl[h] = split(jnp.where(on, v_j, acc[h] / spacing))

    @pl.when(lead)
    def _():
        def drain_q(ch, carry):
            for s in range(nr):
                pl.when(jnp.logical_and(z >= s, z < nr - 1))(lambda s=s: up(s, z - s, ch).wait_send())
                pl.when(jnp.logical_and(z + s < nr, z > 0))(lambda s=s: down(s, z + s, ch).wait_send())
                side(s, ch).wait_send()
            return carry

        lax.fori_loop(0, CHUNKS, drain_q, 0)

    @pl.when(other)
    def _():
        for b in range(nr):
            y_g(b, slot(b, y)).wait_send()
            for h in range(2):
                mate_g(b, h, slot(b, h)).wait_send()
            pl.when(z != b)(lambda b=b: z_g(b).wait_send())

    def part_at(r, lr):
        return span((2 * r + lr) * nr * thin, nr * thin)

    def total_at(r, xx, h, lr):
        return span((((2 * r + xx) * 2 + h) * 2 + lr) * wide, wide)

    far, near, right = span((1 - y) * width, width), span(y * width, width), pl.ds(2 * width, half)

    def left_mate(r):
        return send(
            qbuf.at[part_at(r, 1 - l), pl.ds(0, 2 * width)], mate_in.at[r], lm_out.at[r], lm_in.at[r], mate
        )

    def left_beside(r):
        return send(qbuf.at[part_at(r, l), far], beside_in.at[r], ly_out.at[r], ly_in.at[r], beside)

    def left_spot(r, k):
        return left_in.at[r // FOLD, k, span(r % FOLD * thin, thin)]

    def left_goal(r, k):
        src = beside_in.at[r, pl.ds(k * thin, thin)]
        return send(src, left_spot(r, z), lz_out.at[r, k], lz_in.at[r, z], goal(k))

    def left_here(r):
        return pltpu.make_async_copy(beside_in.at[r, span(z * thin, thin)], left_spot(r, z), lz_in.at[r, z])

    def total_mate(r):
        src = qbuf.at[span((2 * r + 1 - l) * 4 * wide, 4 * wide), right]
        return send(src, total_in.at[r], om_out.at[r], om_in.at[r], mate)

    def total_mine(r):
        return qbuf.at[span((2 * r + l) * 4 * wide, 4 * wide), right]

    def total_half(r, h):
        return qbuf.at[span(((2 * r + l) * 2 + h) * 2 * wide, 2 * wide), right]

    def total_come(r, h):
        return gbuf.at[span((2 * r + h) * 2 * wide, 2 * wide)]

    def total_cross(r, h):
        return send(total_half(r, h), total_come(r, h), ox_out.at[r, h], ox_in.at[r, h], at(z, y, l, x))

    def total_beside(r, src):
        return send(src, total_y.at[r], oy_out.at[r], oy_in.at[r], beside)

    def end(r, lr):
        spot = out_ref.at[span(r * wide, wide), pl.ds(lr * half, half)]
        return pltpu.make_async_copy(total_y.at[r, pl.ds(lr * wide, wide)], spot, end_out.at[r, lr])

    def left(r):
        def side_of(lr):
            take = span(lr * half + r * thin, thin)
            a_hi = qh[:, take, :].reshape(nr * thin, cols)
            a_lo = ql[:, take, :].reshape(nr * thin, cols)
            for h in range(2):
                qbuf[part_at(r, lr), h * width:(h + 1) * width] = mm3(a_hi, a_lo, sh[h], sl[h], NT)

        side_of(1 - l)
        left_mate(r).start()
        side_of(l)
        left_mate(r).wait_recv()
        qbuf[part_at(r, l), far] += mate_in[r, :, far]
        left_beside(r).start()

    def left_end(r):
        left_beside(r).wait_recv()
        beside_in[r] += qbuf[part_at(r, l), near] + mate_in[r, :, near]
        for k in range(nr):
            pl.when(jnp.logical_or(other, z != k))(lambda k=k: left_goal(r, k).start())
        pl.when(lead)(lambda: left_here(r).start())

    def grad(r):
        for f in range(FOLD):
            for k in range(nr):
                t = r * FOLD + f
                pltpu.make_async_copy(beside_in.at[t, pl.ds(k * thin, thin)], left_spot(t, k), lz_in.at[t, k]).wait()
        a_hi, a_lo = split(jnp.concatenate([left_in[r, k] for k in range(nr)], axis=1))
        both = jnp.concatenate([a_hi, a_lo], axis=0)

        def side_of(xx):
            for h in range(2):
                for lr in range(2):
                    take = slice(lr * half, (lr + 1) * half)
                    most = mm(both, qh[2 * h + xx, take, :], NT)
                    rest = mm(a_hi, ql[2 * h + xx, take, :], NT)
                    qbuf[total_at(r, xx, h, lr), right] = most[:wide] + (most[wide:] + rest)

        side_of(1 - l)
        total_mate(r).start()
        side_of(l)
        total_mate(r).wait_recv()
        total_mine(r)[...] += total_in[r]
        pl.when(lead)(lambda: total_beside(r, total_half(r, 1 - y)).start())

        @pl.when(other)
        def _():
            total_cross(r, 1 - y).start()
            total_cross(r, y).start()

    def grad_pass(r):
        @pl.when(other)
        def _():
            total_cross(r, 1 - y).wait_recv()
            total_beside(r, total_come(r, 1 - y)).start()

    def grad_end(r):
        total_beside(r, total_come(r, 1 - y)).wait_recv()

        @pl.when(lead)
        def _():
            total_y[r] += total_half(r, y)[...]

        @pl.when(other)
        def _():
            total_cross(r, y).wait_recv()
            total_y[r] += total_come(r, y)[...]

        for lr in range(2):
            end(r, lr).start()

    def one(r, carry):
        left(r)
        return carry

    def two(r, carry):
        @pl.when(r < ROUNDS)
        def _():
            for f in range(FOLD):
                left_end(r * FOLD + f)
        pl.when(jnp.logical_and(r >= 1, r <= ROUNDS))(lambda: grad(r - 1))
        pl.when(r >= 2)(lambda: grad_pass(r - 2))
        return carry

    def three(r, carry):
        grad_end(r)
        return carry

    def drain_left(r, carry):
        left_mate(r).wait_send()
        left_beside(r).wait_send()
        for k in range(nr):
            pl.when(jnp.logical_or(other, z != k))(lambda k=k: left_goal(r, k).wait_send())
        return carry

    def drain_total(r, carry):
        total_mate(r).wait_send()
        for h in range(2):
            pl.when(other)(lambda h=h: total_cross(r, h).wait_send())
        total_beside(r, total_come(r, 1 - y)).wait_send()
        for lr in range(2):
            end(r, lr).wait()
        return carry

    lax.fori_loop(0, GRAINS, one, 0)
    lax.fori_loop(0, ROUNDS + 2, two, 0)
    lax.fori_loop(0, ROUNDS, three, 0)

    lax.fori_loop(0, GRAINS, drain_left, 0)
    lax.fori_loop(0, ROUNDS, drain_total, 0)


def chip_pairs(basis, basis_grad, value_grad, ranks, offsets):
    nr, nc = lax.axis_size("row"), lax.axis_size("col")
    block, cols = basis.shape
    width = cols // nr
    half = block // 2
    thin, wide = half // GRAINS, half // ROUNDS
    f32, bf16, dma = jnp.float32, jnp.bfloat16, pltpu.SemaphoreType.DMA
    anywhere, vmem = pl.BlockSpec(memory_space=pl.ANY), pl.BlockSpec(memory_space=pltpu.VMEM)
    whole = (nr, block, cols)
    flat = (nc, 1, cols)
    chunked, grains, rounds = dma((nr, CHUNKS)), dma((GRAINS,)), dma((ROUNDS,))
    return pl.pallas_call(
        functools.partial(chip_kernel, nr),
        out_shape=jax.ShapeDtypeStruct((half, cols), f32),
        in_specs=[anywhere, anywhere, vmem, vmem, vmem],
        out_specs=anywhere,
        scratch_shapes=[
            pltpu.VMEM((nr * block, cols), f32), pltpu.VMEM((nr * block, 2 * width), f32),
            pltpu.VMEM(whole, bf16), pltpu.VMEM(whole, bf16), pltpu.VMEM((2, width, cols), f32),
            pltpu.VMEM((2, width, cols), bf16), pltpu.VMEM((2, width, cols), bf16),
            pltpu.VMEM((GRAINS, nr * thin, 2 * width), f32), pltpu.VMEM((GRAINS, nr * thin, width), f32),
            pltpu.VMEM((ROUNDS, nr, wide, width), f32), pltpu.VMEM((ROUNDS, 4 * wide, half), f32),
            pltpu.VMEM((ROUNDS, 2 * wide, half), f32),
            chunked, chunked, chunked, chunked,
            dma((nr,)), dma((nr,)), dma((nr,)), dma((nr,)), dma((nr, 2)), dma((nr, 2)),
            grains, grains, grains, grains, dma((GRAINS, nr)), dma((GRAINS, nr)),
            rounds, rounds, dma((ROUNDS, 2)), dma((ROUNDS, 2)), rounds, rounds, dma((ROUNDS, 2)),
        ],
        compiler_params=pltpu.CompilerParams(
            collective_id=0, has_side_effects=True, vmem_limit_bytes=VMEM_BYTES
        ),
        name="chip_pairs",
    )(basis, basis_grad, ranks.reshape(flat), offsets.reshape(flat), value_grad.reshape(flat))


def dot(a, b, dims):
    return lax.dot_general(
        a, b, (dims, ((), ())), precision=lax.Precision.HIGH, preferred_element_type=jnp.float32
    )


def flip(v, axis, q):
    n = lax.axis_size(axis)
    return lax.ppermute(v, axis, [(i, i ^ q) for i in range(n)])


def shift(v, axis, d):
    if d == 0:
        return v
    n = lax.axis_size(axis)
    return lax.ppermute(v, axis, [(i, (i + d) % n) for i in range(n)])


def gather_begin(v):
    n = lax.axis_size("col")
    if n != 4:
        return [flip(v, "col", q) for q in range(1, n)]
    half = v.shape[0] // 2
    a, b = v[:half], v[half:]
    return [flip(a, "col", 1), flip(b, "col", 2), flip(a, "col", 2), flip(b, "col", 1)]


def gather_end(v, first):
    if lax.axis_size("col") != 4:
        return [v] + first
    a1, b2, a2, b1 = first
    a3, b3 = flip(a1, "col", 2), flip(b2, "col", 1)
    return [v] + [jnp.concatenate(pair) for pair in ((a1, b1), (a2, b2), (a3, b3))]


def scatter_cols(part, rows):
    n = lax.axis_size("col")
    order = (3, 1, 2, 0) if n == 4 else tuple(range(1, n)) + (0,)
    term = {q: lax.optimization_barrier(part(q)) for q in order}
    if n != 4:
        moved = [flip(term[q], "col", q) for q in range(1, n)]
        total = term[0]
        for v in moved:
            total = total + v
        return total, moved[0]
    half = rows // 2
    pa = {q: v[:half] for q, v in term.items()}
    pb = {q: v[half:] for q, v in term.items()}
    moved = flip(pa[3], "col", 1)
    a2 = pa[2] + moved
    b1 = pb[1] + flip(pb[3], "col", 2)
    a0 = pa[0] + flip(pa[1], "col", 1)
    b0 = pb[0] + flip(pb[2], "col", 2)
    return jnp.concatenate([a0 + flip(a2, "col", 2), b0 + flip(b1, "col", 1)]), moved


def swap_layers(mine, axis):
    if lax.axis_size("layer") != 2:
        return lax.all_gather(mine, "layer", axis=axis, tiled=True)
    other = flip(mine, "layer", 1)
    first = lax.axis_index("layer") == 0
    return jnp.concatenate([jnp.where(first, mine, other), jnp.where(first, other, mine)], axis=axis)


def on_device(basis, basis_grad, value_grad, ranks, offsets):
    rows_blk, cols_blk = basis.shape
    nr, nc, nl = (lax.axis_size(a) for a in ("row", "col", "layer"))
    row_id, col_id, layer_id = (lax.axis_index(a) for a in ("row", "col", "layer"))
    width = cols_blk // (nr * nl)
    half = rows_blk // nl

    pieces = [None] * nr
    for d in range(nr):
        begin = (lax.rem(row_id + d, nr) * nl + layer_id) * width
        piece = lax.dynamic_slice_in_dim(basis_grad, begin, width, 1)
        pieces[(nr - d) % nr] = shift(piece, "row", d)

    mine = lax.dynamic_slice_in_dim(basis, layer_id * half, half, 0)
    up, down = [mine], [mine]
    for s in range(1, nr):
        up.append(lax.ppermute(up[-1], "row", [(i, i + 1) for i in range(s - 1, nr - 1)]))
        down.append(lax.ppermute(down[-1], "row", [(i, i - 1) for i in range(1, nr - s + 1)]))
        if s == 1:
            up[1], down[1], pieces = lax.optimization_barrier((up[1], down[1], pieces))
            pieces = jnp.concatenate(pieces)
            begun = gather_begin(pieces)
        if s == 2:
            up[2], down[2], begun = lax.optimization_barrier((up[2], down[2], begun))
    cotangent = jnp.concatenate(gather_end(pieces, begun), axis=1).reshape(nr, rows_blk, nc * width)
    vectors = [basis]
    for e in range(1, nr):
        block = jnp.where(row_id + e < nr, down[e], up[nr - e])
        vectors.append(swap_layers(block, 0))

    inner = dot(vectors[0], cotangent[0], ((0,), (0,)))
    for e in sorted(range(1, nr), key=lambda e: min(e, nr - e)):
        inner = inner + dot(vectors[e], cotangent[e], ((0,), (0,)))

    eigen = 4.0 * ranks.astype(jnp.float32) + offsets.astype(jnp.float32)
    place = row_id * nl + layer_id

    def columns(v):
        mine = lax.dynamic_index_in_dim(v.reshape(nc, nr * nl, width), place, 1, keepdims=False)
        return jnp.concatenate([lax.dynamic_index_in_dim(mine, col_id ^ q, 0, keepdims=False) for q in range(nc)])

    row_index = col_id * cols_blk + jnp.arange(cols_blk, dtype=jnp.int32)
    col_index = columns(jnp.arange(nc * cols_blk, dtype=jnp.int32))
    eigen_rows = lax.dynamic_slice_in_dim(eigen, col_id * cols_blk, cols_blk, 0)
    on_diagonal = row_index[:, None] == col_index[None, :]
    spacing = columns(eigen)[None, :] - eigen_rows[:, None]
    scaled = jnp.where(
        on_diagonal, columns(value_grad)[None, :], inner / jnp.where(on_diagonal, jnp.float32(1.0), spacing)
    )

    arrived = [None] * nr
    order = sorted(range(nr), key=lambda e: -min(e, nr - e))
    groups = [g for g in (order[:nr // 2 - 1], order[nr // 2 - 1:nr - 1], order[nr - 1:]) if g]
    factor = scaled
    for group in groups:
        product = dot(jnp.concatenate([vectors[e] for e in group]), factor, ((1,), (0,)))
        product = lax.optimization_barrier(product)
        summed, first = scatter_cols(lambda q: product[:, q * width:(q + 1) * width], product.shape[0])
        factor, first = lax.optimization_barrier((factor, first))
        for i, e in enumerate(group):
            arrived[e] = shift(summed[i * rows_blk:(i + 1) * rows_blk], "row", e)
    own = []
    for e in range(nr):
        keep = lax.dynamic_slice_in_dim(arrived[e], layer_id * half, half, 0)
        if nl == 1:
            own.append(keep)
            continue
        give = lax.dynamic_slice_in_dim(arrived[e], (1 - layer_id) * half, half, 0)
        other = flip(give, "layer", 1)
        first = layer_id == 0
        own.append(jnp.concatenate([jnp.where(first, keep, other), jnp.where(first, other, keep)], axis=1))
    own = jnp.stack(own)
    left = jnp.concatenate(
        [lax.dynamic_index_in_dim(own, lax.rem(row_id - r + nr, nr), 0, keepdims=False) for r in range(nr)], axis=1
    )

    stack = jnp.stack(vectors)

    def grad_part(q):
        e = lax.rem((col_id ^ q) - row_id + nr, nr)
        block = lax.dynamic_index_in_dim(stack, e, 0, keepdims=False)
        return dot(left, block, ((1,), (1,)))

    return scatter_cols(grad_part, half)[0]


def solution(mesh):
    placed = (P("row", "col"), P("row", "col"), P(), P(), P())
    pairs = (mesh.shape["row"], mesh.shape["col"], mesh.shape["layer"]) == (4, 4, 2)
    return jax.shard_map(
        chip_pairs if pairs else on_device, mesh=mesh, in_specs=placed, out_specs=P(("row", "layer"), "col"), check_vma=False
    )
```

```python
import functools

import jax
import jax.numpy as jnp
from jax import lax
from jax.experimental import pallas as pl
from jax.experimental.pallas import tpu as pltpu
from jax.sharding import PartitionSpec as P


MESH = pl.DeviceIdType.MESH
CHUNKS = 8
GRAINS = 4
ROUNDS = 4
FOLD = GRAINS // ROUNDS
VMEM_BYTES = 63 * 1024 * 1024


def send(src, dst, send_sem, recv_sem, where):
    return pltpu.make_async_remote_copy(
        src_ref=src, dst_ref=dst, send_sem=send_sem, recv_sem=recv_sem, device_id=where, device_id_type=MESH
    )


def greet(places):
    barrier = pltpu.get_barrier_semaphore()
    for where in places:
        pl.semaphore_signal(barrier, inc=1, device_id=where, device_id_type=MESH)
    pl.semaphore_wait(barrier, len(places))


def split(v):
    high = v.astype(jnp.bfloat16)
    return high, (v - high.astype(jnp.float32)).astype(jnp.bfloat16)


def mm(a, b, dims):
    return lax.dot_general(a, b, (dims, ((), ())), preferred_element_type=jnp.float32)


def mm3(a_hi, a_lo, b_hi, b_lo, dims):
    return mm(a_hi, b_hi, dims) + (mm(a_hi, b_lo, dims) + mm(a_lo, b_hi, dims))


NN = ((1,), (0,))
NT = ((1,), (1,))


def place(nr):
    z, c, l = lax.axis_index("row"), lax.axis_index("col"), lax.axis_index("layer")
    return z, c // 2, c % 2, l


def at(z, y, x, l):
    return {"row": z, "col": 2 * y + x, "layer": l}


def chip_kernel(nr, q_ref, g_ref, ranks_ref, offsets_ref, v_ref, out_ref,
                qbuf, gbuf, qh, ql, acc, sh, sl, mate_in, beside_in, left_in, total_in, total_y,
                q_in, up_out, down_out, x_out, gz_out, gz_in, gy_out, gy_in, gl_out, gl_in,
                lm_out, lm_in, ly_out, ly_in, lz_out, lz_in, om_out, om_in, ox_out, ox_in, oy_out, oy_in, end_out):
    z, y, x, l = place(nr)
    lead = l == x
    other = jnp.logical_not(lead)
    block, cols = q_ref.shape
    rows = block // CHUNKS
    width = cols // nr
    half = block // 2
    thin, wide = half // GRAINS, half // ROUNDS
    across, beside, mate = at(z, y, 1 - x, l), at(z, 1 - y, x, l), at(z, y, x, 1 - l)
    goal = lambda k: at(k, y, l, x)
    line = [at(lax.rem(z + d, nr), y, x, l) for d in range(1, nr)] + [across, beside, mate]
    pl.when(lead)(lambda: greet(line))
    pl.when(other)(lambda: greet(line + [goal(lax.rem(z + d, nr)) for d in range(nr)]))

    def span(start, size):
        return pl.ds(pl.multiple_of(start, size), size)

    def local_q(ch):
        return pltpu.make_async_copy(
            q_ref.at[span(ch * rows, rows)], qbuf.at[span(z * block + ch * rows, rows)], q_in.at[z, ch]
        )

    def pass_q(s, b, ch, out, where, own):
        spot = qbuf.at[span(b * block + ch * rows, rows)]
        src = q_ref.at[span(ch * rows, rows)] if own else spot
        return send(src, spot, out.at[s, ch], q_in.at[b, ch], where)

    def up(s, b, ch, own=False):
        return pass_q(s, b, ch, up_out, at(z + 1, y, x, l), own)

    def down(s, b, ch, own=False):
        return pass_q(s, b, ch, down_out, at(z - 1, y, x, l), own)

    def side(b, ch, own=False):
        return pass_q(b, b, ch, x_out, across, own)

    def await_q(b, ch):
        pltpu.make_async_copy(
            q_ref.at[span(ch * rows, rows)], qbuf.at[span(b * block + ch * rows, rows)], q_in.at[b, ch]
        ).wait()

    def slot(b, h):
        return gbuf.at[span(b * block, block), span(h * width, width)]

    def own_g(k):
        return g_ref.at[:, span(k * width, width)]

    def z_g(k):
        return send(own_g(k), slot(z, y), gz_out.at[k], gz_in.at[z], at(k, y, x, l))

    def y_g(b, src):
        return send(src, slot(b, y), gy_out.at[b], gy_in.at[b], beside)

    def mate_g(b, h, src):
        return send(src, slot(b, h), gl_out.at[b, h], gl_in.at[b, h], mate)

    def own_g_copy():
        return pltpu.make_async_copy(own_g(z), slot(z, y), gz_in.at[z])

    def await_z_g(b):
        pltpu.make_async_copy(own_g(0), slot(b, y), gz_in.at[b]).wait()

    def await_y_g(b):
        pltpu.make_async_copy(own_g(0), slot(b, 1 - y), gy_in.at[b]).wait()

    @pl.when(lead)
    def _():
        for ch in range(CHUNKS):
            side(z, ch, True).start()
            pl.when(z < nr - 1)(lambda ch=ch: up(0, z, ch, True).start())
            pl.when(z > 0)(lambda ch=ch: down(0, z, ch, True).start())
            local_q(ch).start()

    @pl.when(other)
    def _():
        for d in range(1, nr):
            pl.when(z + d < nr)(lambda d=d: z_g(z + d).start())
            pl.when(z - d >= 0)(lambda d=d: z_g(z - d).start())
        y_g(z, own_g(z)).start()
        mate_g(z, y, own_g(z)).start()
        own_g_copy().start()
        await_y_g(z)
        mate_g(z, 1 - y, slot(z, 1 - y)).start()
        for d in range(1, nr):
            for step in (-d, d):
                b = z + step

                @pl.when(jnp.logical_and(b >= 0, b < nr))
                def _(b=b):
                    await_z_g(b)
                    y_g(b, slot(b, y)).start()
                    mate_g(b, y, slot(b, y)).start()
            for step in (-d, d):
                b = z + step

                @pl.when(jnp.logical_and(b >= 0, b < nr))
                def _(b=b):
                    await_y_g(b)
                    mate_g(b, 1 - y, slot(b, 1 - y)).start()
        await_z_g(z)

    acc[...] = jnp.zeros_like(acc)

    def absorb(s, b, ch):
        pl.when(jnp.logical_or(other, s == 0))(lambda: await_q(b, ch))

        @pl.when(jnp.logical_and(lead, ch == 0))
        def _():
            for h in range(2):
                pltpu.make_async_copy(own_g(0), slot(b, h), gl_in.at[b, h]).wait()

        part, taken = span(ch * rows, rows), span(b * block + ch * rows, rows)
        high, low = split(qbuf[taken, :])
        qh[b, part, :] = high
        ql[b, part, :] = low
        for h in range(2):
            g_hi, g_lo = split(gbuf[taken, h * width:(h + 1) * width].T)
            acc[h] += mm3(g_hi, g_lo, high, low, NN)

    def forward(s, ch):
        @pl.when(jnp.logical_and(lead, z >= s))
        def _():
            await_q(z - s, ch)
            pl.when(z < nr - 1)(lambda: up(s, z - s, ch).start())
            side(z - s, ch).start()

        @pl.when(jnp.logical_and(lead, z + s < nr))
        def _():
            await_q(z + s, ch)
            pl.when(z > 0)(lambda: down(s, z + s, ch).start())
            side(z + s, ch).start()

    def absorb_at(s, ch):
        pl.when(z >= s)(lambda: absorb(s, z - s, ch))
        if s > 0:
            pl.when(z + s < nr)(lambda: absorb(s, z + s, ch))

    for s in range(1, nr):
        def step(ch, carry, s=s):
            forward(s, ch)
            absorb_at(s - 1, ch)
            if s == nr - 1:
                absorb_at(s, ch)
            return carry

        lax.fori_loop(0, CHUNKS, step, 0)

    def eigen(k, where):
        return 4.0 * ranks_ref[k, :, where].astype(jnp.float32) + offsets_ref[k, :, where].astype(jnp.float32)

    e_i = eigen(2 * y + l, slice(None))
    i_at = (2 * y + l) * cols + lax.broadcasted_iota(jnp.int32, (width, cols), 1)
    for h in range(2):
        j_cols = span(z * width, width)
        upright = lambda v: jnp.broadcast_to(v, (128, width)).T[:, :1]
        e_j, v_j = upright(eigen(2 * h + x, j_cols)), upright(v_ref[2 * h + x, :, j_cols])
        j_at = (2 * h + x) * cols + z * width + lax.broadcasted_iota(jnp.int32, (width, cols), 0)
        on = i_at == j_at
        spacing = jnp.where(on, jnp.float32(1.0), e_j - e_i)
        sh[h], sl[h] = split(jnp.where(on, v_j, acc[h] / spacing))

    @pl.when(lead)
    def _():
        def drain_q(ch, carry):
            for s in range(nr):
                pl.when(jnp.logical_and(z >= s, z < nr - 1))(lambda s=s: up(s, z - s, ch).wait_send())
                pl.when(jnp.logical_and(z + s < nr, z > 0))(lambda s=s: down(s, z + s, ch).wait_send())
                side(s, ch).wait_send()
            return carry

        lax.fori_loop(0, CHUNKS, drain_q, 0)

    @pl.when(other)
    def _():
        for b in range(nr):
            y_g(b, slot(b, y)).wait_send()
            for h in range(2):
                mate_g(b, h, slot(b, h)).wait_send()
            pl.when(z != b)(lambda b=b: z_g(b).wait_send())

    def part_at(r, lr):
        return span((2 * r + lr) * nr * thin, nr * thin)

    def total_at(r, xx, h, lr):
        return span((((2 * r + xx) * 2 + h) * 2 + lr) * wide, wide)

    far, near, right = span((1 - y) * width, width), span(y * width, width), pl.ds(2 * width, half)

    def left_mate(r):
        return send(
            qbuf.at[part_at(r, 1 - l), pl.ds(0, 2 * width)], mate_in.at[r], lm_out.at[r], lm_in.at[r], mate
        )

    def left_beside(r):
        return send(qbuf.at[part_at(r, l), far], beside_in.at[r], ly_out.at[r], ly_in.at[r], beside)

    def left_spot(r, k):
        return left_in.at[r // FOLD, k, span(r % FOLD * thin, thin)]

    def left_goal(r, k):
        src = beside_in.at[r, pl.ds(k * thin, thin)]
        return send(src, left_spot(r, z), lz_out.at[r, k], lz_in.at[r, z], goal(k))

    def left_here(r):
        return pltpu.make_async_copy(beside_in.at[r, span(z * thin, thin)], left_spot(r, z), lz_in.at[r, z])

    def total_mate(r):
        src = qbuf.at[span((2 * r + 1 - l) * 4 * wide, 4 * wide), right]
        return send(src, total_in.at[r], om_out.at[r], om_in.at[r], mate)

    def total_mine(r):
        return qbuf.at[span((2 * r + l) * 4 * wide, 4 * wide), right]

    def total_half(r, h):
        return qbuf.at[span(((2 * r + l) * 2 + h) * 2 * wide, 2 * wide), right]

    def total_come(r, h):
        return gbuf.at[span((2 * r + h) * 2 * wide, 2 * wide)]

    def total_cross(r, h):
        return send(total_half(r, h), total_come(r, h), ox_out.at[r, h], ox_in.at[r, h], at(z, y, l, x))

    def total_beside(r, src):
        return send(src, total_y.at[r], oy_out.at[r], oy_in.at[r], beside)

    def end(r, lr):
        spot = out_ref.at[span(r * wide, wide), pl.ds(lr * half, half)]
        return pltpu.make_async_copy(total_y.at[r, pl.ds(lr * wide, wide)], spot, end_out.at[r, lr])

    def left(r):
        def side_of(lr):
            take = span(lr * half + r * thin, thin)
            a_hi = qh[:, take, :].reshape(nr * thin, cols)
            a_lo = ql[:, take, :].reshape(nr * thin, cols)
            for h in range(2):
                qbuf[part_at(r, lr), h * width:(h + 1) * width] = mm3(a_hi, a_lo, sh[h], sl[h], NT)

        side_of(1 - l)
        left_mate(r).start()
        side_of(l)
        left_mate(r).wait_recv()
        qbuf[part_at(r, l), far] += mate_in[r, :, far]
        left_beside(r).start()

    def left_end(r):
        left_beside(r).wait_recv()
        beside_in[r] += qbuf[part_at(r, l), near] + mate_in[r, :, near]
        for k in range(nr):
            pl.when(jnp.logical_or(other, z != k))(lambda k=k: left_goal(r, k).start())
        pl.when(lead)(lambda: left_here(r).start())

    def grad(r):
        for f in range(FOLD):
            for k in range(nr):
                t = r * FOLD + f
                pltpu.make_async_copy(beside_in.at[t, pl.ds(k * thin, thin)], left_spot(t, k), lz_in.at[t, k]).wait()
        a_hi, a_lo = split(jnp.concatenate([left_in[r, k] for k in range(nr)], axis=1))
        both = jnp.concatenate([a_hi, a_lo], axis=0)

        def side_of(xx):
            for h in range(2):
                for lr in range(2):
                    take = slice(lr * half, (lr + 1) * half)
                    most = mm(both, qh[2 * h + xx, take, :], NT)
                    rest = mm(a_hi, ql[2 * h + xx, take, :], NT)
                    qbuf[total_at(r, xx, h, lr), right] = most[:wide] + (most[wide:] + rest)

        side_of(1 - l)
        total_mate(r).start()
        side_of(l)
        total_mate(r).wait_recv()
        total_mine(r)[...] += total_in[r]
        pl.when(lead)(lambda: total_beside(r, total_half(r, 1 - y)).start())

        @pl.when(other)
        def _():
            total_cross(r, 1 - y).start()
            total_cross(r, y).start()

    def grad_pass(r):
        @pl.when(other)
        def _():
            total_cross(r, 1 - y).wait_recv()
            total_beside(r, total_come(r, 1 - y)).start()

    def grad_end(r):
        total_beside(r, total_come(r, 1 - y)).wait_recv()

        @pl.when(lead)
        def _():
            total_y[r] += total_half(r, y)[...]

        @pl.when(other)
        def _():
            total_cross(r, y).wait_recv()
            total_y[r] += total_come(r, y)[...]

        for lr in range(2):
            end(r, lr).start()

    def one(r, carry):
        left(r)
        return carry

    def two(r, carry):
        @pl.when(r < ROUNDS)
        def _():
            for f in range(FOLD):
                left_end(r * FOLD + f)
        pl.when(jnp.logical_and(r >= 1, r <= ROUNDS))(lambda: grad(r - 1))
        pl.when(r >= 2)(lambda: grad_pass(r - 2))
        return carry

    def three(r, carry):
        grad_end(r)
        return carry

    def drain_left(r, carry):
        left_mate(r).wait_send()
        left_beside(r).wait_send()
        for k in range(nr):
            pl.when(jnp.logical_or(other, z != k))(lambda k=k: left_goal(r, k).wait_send())
        return carry

    def drain_total(r, carry):
        total_mate(r).wait_send()
        for h in range(2):
            pl.when(other)(lambda h=h: total_cross(r, h).wait_send())
        total_beside(r, total_come(r, 1 - y)).wait_send()
        for lr in range(2):
            end(r, lr).wait()
        return carry

    lax.fori_loop(0, GRAINS, one, 0)
    lax.fori_loop(0, ROUNDS + 2, two, 0)
    lax.fori_loop(0, ROUNDS, three, 0)

    lax.fori_loop(0, GRAINS, drain_left, 0)
    lax.fori_loop(0, ROUNDS, drain_total, 0)


def chip_pairs(basis, basis_grad, value_grad, ranks, offsets):
    nr, nc = lax.axis_size("row"), lax.axis_size("col")
    block, cols = basis.shape
    width = cols // nr
    half = block // 2
    thin, wide = half // GRAINS, half // ROUNDS
    f32, bf16, dma = jnp.float32, jnp.bfloat16, pltpu.SemaphoreType.DMA
    anywhere, vmem = pl.BlockSpec(memory_space=pl.ANY), pl.BlockSpec(memory_space=pltpu.VMEM)
    whole = (nr, block, cols)
    flat = (nc, 1, cols)
    chunked, grains, rounds = dma((nr, CHUNKS)), dma((GRAINS,)), dma((ROUNDS,))
    return pl.pallas_call(
        functools.partial(chip_kernel, nr),
        out_shape=jax.ShapeDtypeStruct((half, cols), f32),
        in_specs=[anywhere, anywhere, vmem, vmem, vmem],
        out_specs=anywhere,
        scratch_shapes=[
            pltpu.VMEM((nr * block, cols), f32), pltpu.VMEM((nr * block, 2 * width), f32),
            pltpu.VMEM(whole, bf16), pltpu.VMEM(whole, bf16), pltpu.VMEM((2, width, cols), f32),
            pltpu.VMEM((2, width, cols), bf16), pltpu.VMEM((2, width, cols), bf16),
            pltpu.VMEM((GRAINS, nr * thin, 2 * width), f32), pltpu.VMEM((GRAINS, nr * thin, width), f32),
            pltpu.VMEM((ROUNDS, nr, wide, width), f32), pltpu.VMEM((ROUNDS, 4 * wide, half), f32),
            pltpu.VMEM((ROUNDS, 2 * wide, half), f32),
            chunked, chunked, chunked, chunked,
            dma((nr,)), dma((nr,)), dma((nr,)), dma((nr,)), dma((nr, 2)), dma((nr, 2)),
            grains, grains, grains, grains, dma((GRAINS, nr)), dma((GRAINS, nr)),
            rounds, rounds, dma((ROUNDS, 2)), dma((ROUNDS, 2)), rounds, rounds, dma((ROUNDS, 2)),
        ],
        compiler_params=pltpu.CompilerParams(
            collective_id=0, has_side_effects=True, vmem_limit_bytes=VMEM_BYTES
        ),
        name="chip_pairs",
    )(basis, basis_grad, ranks.reshape(flat), offsets.reshape(flat), value_grad.reshape(flat))


def dot(a, b, dims):
    return lax.dot_general(
        a, b, (dims, ((), ())), precision=lax.Precision.HIGH, preferred_element_type=jnp.float32
    )


def flip(v, axis, q):
    n = lax.axis_size(axis)
    return lax.ppermute(v, axis, [(i, i ^ q) for i in range(n)])


def shift(v, axis, d):
    if d == 0:
        return v
    n = lax.axis_size(axis)
    return lax.ppermute(v, axis, [(i, (i + d) % n) for i in range(n)])


def gather_begin(v):
    n = lax.axis_size("col")
    if n != 4:
        return [flip(v, "col", q) for q in range(1, n)]
    half = v.shape[0] // 2
    a, b = v[:half], v[half:]
    return [flip(a, "col", 1), flip(b, "col", 2), flip(a, "col", 2), flip(b, "col", 1)]


def gather_end(v, first):
    if lax.axis_size("col") != 4:
        return [v] + first
    a1, b2, a2, b1 = first
    a3, b3 = flip(a1, "col", 2), flip(b2, "col", 1)
    return [v] + [jnp.concatenate(pair) for pair in ((a1, b1), (a2, b2), (a3, b3))]


def scatter_cols(part, rows):
    n = lax.axis_size("col")
    order = (3, 1, 2, 0) if n == 4 else tuple(range(1, n)) + (0,)
    term = {q: lax.optimization_barrier(part(q)) for q in order}
    if n != 4:
        moved = [flip(term[q], "col", q) for q in range(1, n)]
        total = term[0]
        for v in moved:
            total = total + v
        return total, moved[0]
    half = rows // 2
    pa = {q: v[:half] for q, v in term.items()}
    pb = {q: v[half:] for q, v in term.items()}
    moved = flip(pa[3], "col", 1)
    a2 = pa[2] + moved
    b1 = pb[1] + flip(pb[3], "col", 2)
    a0 = pa[0] + flip(pa[1], "col", 1)
    b0 = pb[0] + flip(pb[2], "col", 2)
    return jnp.concatenate([a0 + flip(a2, "col", 2), b0 + flip(b1, "col", 1)]), moved


def swap_layers(mine, axis):
    if lax.axis_size("layer") != 2:
        return lax.all_gather(mine, "layer", axis=axis, tiled=True)
    other = flip(mine, "layer", 1)
    first = lax.axis_index("layer") == 0
    return jnp.concatenate([jnp.where(first, mine, other), jnp.where(first, other, mine)], axis=axis)


def on_device(basis, basis_grad, value_grad, ranks, offsets):
    rows_blk, cols_blk = basis.shape
    nr, nc, nl = (lax.axis_size(a) for a in ("row", "col", "layer"))
    row_id, col_id, layer_id = (lax.axis_index(a) for a in ("row", "col", "layer"))
    width = cols_blk // (nr * nl)
    half = rows_blk // nl

    pieces = [None] * nr
    for d in range(nr):
        begin = (lax.rem(row_id + d, nr) * nl + layer_id) * width
        piece = lax.dynamic_slice_in_dim(basis_grad, begin, width, 1)
        pieces[(nr - d) % nr] = shift(piece, "row", d)

    mine = lax.dynamic_slice_in_dim(basis, layer_id * half, half, 0)
    up, down = [mine], [mine]
    for s in range(1, nr):
        up.append(lax.ppermute(up[-1], "row", [(i, i + 1) for i in range(s - 1, nr - 1)]))
        down.append(lax.ppermute(down[-1], "row", [(i, i - 1) for i in range(1, nr - s + 1)]))
        if s == 1:
            up[1], down[1], pieces = lax.optimization_barrier((up[1], down[1], pieces))
            pieces = jnp.concatenate(pieces)
            begun = gather_begin(pieces)
        if s == 2:
            up[2], down[2], begun = lax.optimization_barrier((up[2], down[2], begun))
    cotangent = jnp.concatenate(gather_end(pieces, begun), axis=1).reshape(nr, rows_blk, nc * width)
    vectors = [basis]
    for e in range(1, nr):
        block = jnp.where(row_id + e < nr, down[e], up[nr - e])
        vectors.append(swap_layers(block, 0))

    inner = dot(vectors[0], cotangent[0], ((0,), (0,)))
    for e in sorted(range(1, nr), key=lambda e: min(e, nr - e)):
        inner = inner + dot(vectors[e], cotangent[e], ((0,), (0,)))

    eigen = 4.0 * ranks.astype(jnp.float32) + offsets.astype(jnp.float32)
    place = row_id * nl + layer_id

    def columns(v):
        mine = lax.dynamic_index_in_dim(v.reshape(nc, nr * nl, width), place, 1, keepdims=False)
        return jnp.concatenate([lax.dynamic_index_in_dim(mine, col_id ^ q, 0, keepdims=False) for q in range(nc)])

    row_index = col_id * cols_blk + jnp.arange(cols_blk, dtype=jnp.int32)
    col_index = columns(jnp.arange(nc * cols_blk, dtype=jnp.int32))
    eigen_rows = lax.dynamic_slice_in_dim(eigen, col_id * cols_blk, cols_blk, 0)
    on_diagonal = row_index[:, None] == col_index[None, :]
    spacing = columns(eigen)[None, :] - eigen_rows[:, None]
    scaled = jnp.where(
        on_diagonal, columns(value_grad)[None, :], inner / jnp.where(on_diagonal, jnp.float32(1.0), spacing)
    )

    arrived = [None] * nr
    order = sorted(range(nr), key=lambda e: -min(e, nr - e))
    groups = [g for g in (order[:nr // 2 - 1], order[nr // 2 - 1:nr - 1], order[nr - 1:]) if g]
    factor = scaled
    for group in groups:
        product = dot(jnp.concatenate([vectors[e] for e in group]), factor, ((1,), (0,)))
        product = lax.optimization_barrier(product)
        summed, first = scatter_cols(lambda q: product[:, q * width:(q + 1) * width], product.shape[0])
        factor, first = lax.optimization_barrier((factor, first))
        for i, e in enumerate(group):
            arrived[e] = shift(summed[i * rows_blk:(i + 1) * rows_blk], "row", e)
    own = []
    for e in range(nr):
        keep = lax.dynamic_slice_in_dim(arrived[e], layer_id * half, half, 0)
        if nl == 1:
            own.append(keep)
            continue
        give = lax.dynamic_slice_in_dim(arrived[e], (1 - layer_id) * half, half, 0)
        other = flip(give, "layer", 1)
        first = layer_id == 0
        own.append(jnp.concatenate([jnp.where(first, keep, other), jnp.where(first, other, keep)], axis=1))
    own = jnp.stack(own)
    left = jnp.concatenate(
        [lax.dynamic_index_in_dim(own, lax.rem(row_id - r + nr, nr), 0, keepdims=False) for r in range(nr)], axis=1
    )

    stack = jnp.stack(vectors)

    def grad_part(q):
        e = lax.rem((col_id ^ q) - row_id + nr, nr)
        block = lax.dynamic_index_in_dim(stack, e, 0, keepdims=False)
        return dot(left, block, ((1,), (1,)))

    return scatter_cols(grad_part, half)[0]


def solution(mesh):
    placed = (P("row", "col"), P("row", "col"), P(), P(), P())
    pairs = (mesh.shape["row"], mesh.shape["col"], mesh.shape["layer"]) == (4, 4, 2)
    return jax.shard_map(
        chip_pairs if pairs else on_device, mesh=mesh, in_specs=placed, out_specs=P(("row", "layer"), "col"), check_vma=False
    )
```
